32 devices in a mesh: exp: 4 (over x, core), patch: 8 (over z, y).
Axes of the slice: x: 2, y: 2, z: 4, core: 2. Of those that a mesh axis runs over, the one named last changes fastest.
Arguments:
- pixels: float32 [4, 256, 128, 128], P('exp', 'patch'), may hold values from -6 to 6
- exposure_of: int32 [4, 256], P('exp', 'patch'), may hold values from 0 to 3
- destination: int32 [4, 256, 1], P('exp', 'patch'), may hold values from 0 to 7; in each aligned block of 32 rows (0 to 31, 32 to 63, ..., all dimensions but the last counted through in order) at most 6 rows name the same one
- tile_slot: int32 [4, 256], P('exp', 'patch'), may hold values from 0 to 63
- psf_left: float32 [4, 4, 128, 128], P('exp'), may hold values from -0.06 to 2.5, as said below
- psf_right: float32 [4, 4, 128, 128], P('exp'), may hold values from -0.06 to 2.5, as said below
- weights: float32 [4, 4], P('exp'), may hold values from 0.2 to 5
Outputs:
- coadd: float32 [8, 1024, 1024], P('patch')
- detection: float32 [8, 1024, 1024], P('patch')
The draws below stay inside these ranges and needn't reach their ends.
Inputs may be any that keep to these rules, and one draw needn't show every extreme that they name: `destination`: the blocks of one device (aligned runs of 32 rows) name each patch at most 6 times; some patch is named exactly 6 times by some device. `tile_slot`: several blocks may share a tile; a tile may have none. `psf_left`: diagonal entries lie in 1.5 to 2.5, the others in -0.06 to 0.06. `psf_right`: diagonal entries lie in 1.5 to 2.5, the others in -0.06 to 0.06.
All inputs are finite; a program needn't handle non-finite values.
Results may differ from the reference program's by a relative error of at most 0.0003.
Values sent between devices are 32-bit elements; how exact they have to be, the bound alone decides.
No kernel may reach another device: no remote copies, remote signals or barrier semaphores. Data moves between devices by JAX's collectives and lax.ppermute only.
A program may use at most 128 MiB of HBM per device.

```python
import math
import jax
import jax.numpy as jnp
import numpy as np
from jax import lax

BS = 128
PATCH_PIX = 1024
BLK = 32
CAP = 6
EXP_DEV = 4
HALO = 4
PCOLS = 4
BLOCKS = 256
N_EXP = 4
N_PATCH = 8


def psf_operator(key):
    diag_key = jax.random.fold_in(key, 11)
    off_key = jax.random.fold_in(key, 12)
    shape = (N_EXP, EXP_DEV, BS, BS)
    offdiag = jax.random.uniform(off_key, shape, jnp.float32, -0.06, 0.06)
    diagonal = jax.random.uniform(diag_key, (N_EXP, EXP_DEV, BS), jnp.float32, 1.5, 2.5)
    eye = jnp.eye(BS, dtype=jnp.float32)
    return offdiag * (1.0 - eye) + eye * diagonal[..., None]


def draw_psf_left(key, part):
    return psf_operator(jax.random.fold_in(key, 101))


def draw_psf_right(key, part):
    return psf_operator(jax.random.fold_in(key, 202))


def with_ends(values, stream_key, smallest, top_value):
    place = [jax.random.randint(jax.random.fold_in(stream_key, axis), (), 0, length) for axis, length in enumerate(values.shape)]
    longest = values.shape.index(max(values.shape))
    beside = place[:longest] + [(place[longest] + 1) % values.shape[longest]] + place[longest + 1:]
    return values.at[tuple(place)].set(smallest).at[tuple(beside)].set(top_value)


def levels(rng, shape, shards, low, high):
    loudness = 1.0
    for position, shards_of in shards:
        heights = jax.random.uniform(jax.random.fold_in(jax.random.fold_in(rng, 6), position), (shards_of,), jnp.float32, low / len(shards), high / len(shards))
        loudness = loudness * jnp.repeat(jnp.exp(heights), shape[position] // shards_of).reshape((-1,) + (1,) * (len(shape) - 1 - position))
    return loudness


def assign_block(stream_key, own, number, rows, number_of, top, most, skew):
    order = jax.random.permutation(stream_key, number_of)
    crowded, ordinary = portions_of(number_of, rows * top, most, skew, True), portions_of(number_of, rows * top, most, skew, False)
    places = jnp.arange(number_of)

    def named(sizes, offset_by):
        used = int((sizes > 0).sum())
        fixed = max(1, used // 4)
        shifted = fixed + (places - fixed + offset_by * (used - fixed)) % max(1, number_of - fixed)
        return jnp.zeros((number_of,), jnp.int32).at[order[jnp.where(places < fixed, places, shifted)]].set(jnp.asarray(sizes, jnp.int32))

    sizes = jnp.where(number % 4 == 0, named(crowded, number // 4), named(ordinary, number - number // 4 - 1))
    mixed = jax.random.permutation(jax.random.fold_in(own, 3), number_of)
    source_of, taker = mixed[0:number_of // 2 * 2:2], mixed[1:number_of // 2 * 2:2]
    margin = jnp.minimum(sizes[source_of] - 1, most - sizes[taker]) // 2
    margin = jnp.where((source_of == order[0]) | (taker == order[0]) | (sizes[taker] == 0), 0, jnp.maximum(margin, 0))
    shifted = jax.random.randint(jax.random.fold_in(own, 4), (number_of // 2,), 0, 1 << 20) % (margin + 1)
    sizes = sizes.at[source_of].add(-shifted).at[taker].add(shifted)
    members = jnp.searchsorted(jnp.cumsum(sizes), jnp.arange(rows * top), side="right").astype(jnp.int32)
    table = members.reshape(top, rows).T
    table = table[jax.random.permutation(jax.random.fold_in(own, 1), rows)]
    offset_by = jax.random.randint(jax.random.fold_in(own, 2), (rows, 1), 0, top)
    return jnp.take_along_axis(table, (jnp.arange(top)[None, :] + offset_by) % top, axis=1)


def portions_of(count, total, bound, skew, full):
    portions = [(1 << 20) // math.isqrt(standing ** skew) + 1 for standing in range(1, count + 1)]
    largest = bound if full else min(bound, max(-(-total // count), total * portions[0] // sum(portions)))
    least = 1 if total - largest >= count - 1 else 0
    holding, surplus = [largest] + [least] * (count - 1), total - largest - least * (count - 1)
    while surplus > 0:
        movable = [i for i in range(1, count) if holding[i] < largest] or [i for i in range(1, count) if holding[i] < bound]
        mass, budget = sum([portions[i] for i in movable]), surplus
        for i in movable:
            extra = min(bound - holding[i], max(1, budget * portions[i] // mass), surplus)
            holding[i] = holding[i] + extra
            surplus = surplus - extra
    return np.array(holding)


def noise(own_key, shape, spread, limit, split=(), kind=jnp.bfloat16):
    result = jax.random.normal(own_key, shape, jnp.float32) * spread
    if len(split) > 0:
        result = levels(own_key, shape, split, -0.22, 0.18) * result
    return jnp.clip(result, min=-limit, max=limit).astype(kind)


def setup_inputs(seed: int = 0) -> dict:
    key_of = jax.random.split(jax.random.key(seed), 8)
    pixels = noise(key_of[0], (N_EXP, BLOCKS, BS, BS), 1.0, 6.0, ((0, 4), (1, 8)), jnp.float32)
    exposure_of = with_ends(jax.random.randint(key_of[1], (N_EXP, BLOCKS), 0, EXP_DEV), jax.random.fold_in(key_of[1], 1), 0, EXP_DEV - 1).astype(jnp.int32)
    destination_keys = jax.random.split(jax.random.fold_in(key_of[2], 1), N_EXP * BLOCKS // BLK)
    destination_turns = jax.random.permutation(jax.random.fold_in(key_of[2], 3), N_EXP * BLOCKS // BLK)
    destination = jax.vmap(lambda own, number: assign_block(jax.random.fold_in(key_of[2], 2), own, number, BLK, N_PATCH, 1, CAP, 2))(destination_keys, destination_turns).reshape((N_EXP, BLOCKS, 1))
    tile_slot = with_ends(jax.random.randint(key_of[3], (N_EXP, BLOCKS), 0, (PATCH_PIX // BS) ** 2), jax.random.fold_in(key_of[3], 1), 0, ((PATCH_PIX // BS) ** 2) - 1).astype(jnp.int32)
    psf_left = draw_psf_left(jax.random.fold_in(key_of[7], 71), 0)
    psf_right = draw_psf_right(jax.random.fold_in(key_of[7], 71), 0)
    weights = jnp.clip(jnp.exp(math.log(5.0) - 3.218876 * jax.random.uniform(key_of[6], (N_EXP, EXP_DEV), jnp.float32) ** levels(key_of[6], (N_EXP, EXP_DEV), ((0, 4),), -0.2, 0.2)), 0.2, 5.0)
    return dict(pixels=pixels, exposure_of=exposure_of, destination=destination, tile_slot=tile_slot, psf_left=psf_left, psf_right=psf_right, weights=weights)


def kernel_taps():
    taps = jnp.arange(-HALO, HALO + 1).astype(jnp.float32)
    values = jnp.exp(-taps * taps / 8.0)
    return values / jnp.sum(values)


def reference(pixels, exposure_of, destination, tile_slot, psf_left, psf_right, weights):
    tiles_side = PATCH_PIX // BS
    n_tiles = tiles_side * tiles_side
    segments = N_PATCH * n_tiles

    def one_row(carry, inputs):
        numer, wsum = carry
        blocks, expo, dest, tiles, left, right, wexp = inputs
        inner = jnp.einsum("bij,bjk->bik", left[expo], blocks, precision=lax.Precision.HIGHEST)
        matched = jnp.einsum("bik,blk->bil", inner, right[expo], precision=lax.Precision.HIGHEST)
        wblock = wexp[expo]
        matched = matched * wblock[:, None, None]
        key = (dest[:, 0] * n_tiles + tiles).astype(jnp.int32)
        numer = numer + jax.ops.segment_sum(matched, key, num_segments=segments)
        wsum = wsum + jax.ops.segment_sum(wblock, key, num_segments=segments)
        return (numer, wsum), None

    start = (jnp.zeros((segments, BS, BS), jnp.float32), jnp.zeros((segments,), jnp.float32))
    (numer, wsum), _ = lax.scan(one_row, start, (pixels, exposure_of, destination, tile_slot, psf_left, psf_right, weights))
    tiles = numer / (wsum + 1.0)[:, None, None]
    patches = tiles.reshape(N_PATCH, tiles_side, tiles_side, BS, BS).transpose(0, 1, 3, 2, 4).reshape(N_PATCH, PATCH_PIX, PATCH_PIX)
    grid_rows = N_PATCH // PCOLS
    tract = patches.reshape(grid_rows, PCOLS, PATCH_PIX, PATCH_PIX).transpose(0, 2, 1, 3).reshape(grid_rows * PATCH_PIX, PCOLS * PATCH_PIX)
    taps = kernel_taps()
    rows_total = tract.shape[0]
    cols_total = tract.shape[1]
    padded = jnp.pad(tract, ((HALO, HALO), (0, 0)))
    vertical = jnp.zeros_like(tract)
    for shift in range(2 * HALO + 1):
        vertical = vertical + taps[shift] * padded[shift:shift + rows_total, :]
    padded = jnp.pad(vertical, ((0, 0), (HALO, HALO)))
    smoothed = jnp.zeros_like(tract)
    for shift in range(2 * HALO + 1):
        smoothed = smoothed + taps[shift] * padded[:, shift:shift + cols_total]
    detection = smoothed.reshape(grid_rows, PATCH_PIX, PCOLS, PATCH_PIX).transpose(0, 2, 1, 3).reshape(N_PATCH, PATCH_PIX, PATCH_PIX)
    return patches, detection
```

```python
import functools

import jax
import jax.numpy as jnp
from jax import lax
from jax.experimental import pallas as pl
from jax.experimental.pallas import tpu as pltpu
from jax.sharding import PartitionSpec as P

PATCH_PIX = 1024
CAP = 6
HALO = 4
PCOLS = 4
SUB = 8
LANES = 128


def kernel_taps():
    taps = jnp.arange(-HALO, HALO + 1).astype(jnp.float32)
    values = jnp.exp(-taps * taps / 8.0)
    return values / jnp.sum(values)


def split(x):
    high = x.astype(jnp.bfloat16)
    return high, (x - high.astype(jnp.float32)).astype(jnp.bfloat16)


def dot(a, b):
    return jnp.dot(a, b, preferred_element_type=jnp.float32)


def message_kernel(steps, n_patch, me, dest, tile, expo, weight, blocks, left, right, *rest):
    outs = rest[: len(steps)]
    lcat, rcat, rlow, slots, counts = rest[len(steps) :]
    count, bs = blocks.shape[0], blocks.shape[1]
    for k in range(left.shape[0]):
        high, low = split(left[k] * weight[k])
        lcat[k, :, :bs] = high
        lcat[k, :, bs:] = low
        high, low = split(right[k].T)
        rcat[k, :bs, :] = high
        rcat[k, bs:, :] = high
        rlow[k] = low
    for q in range(n_patch):
        counts[q] = 0

    def place(b, carry):
        q = dest[b]
        r = counts[q]
        slots[q * CAP + r] = b
        counts[q] = r + 1
        return carry

    lax.fori_loop(0, count, place, 0)
    lane = lax.broadcasted_iota(jnp.int32, (SUB, LANES), 1)
    row = lax.broadcasted_iota(jnp.int32, (SUB, LANES), 0)
    for step, out in zip(steps, outs, strict=True):
        q = me[0] ^ step
        held = counts[q]
        meta = jnp.full((SUB, LANES), -1.0, jnp.float32)
        for r in range(CAP):
            b = jnp.where(r < held, slots[q * CAP + r], 0)
            k = expo[b]
            high, low = split(blocks[b])
            lk = lcat[k]
            inner = dot(lk, jnp.concatenate([high, high], axis=0)) + dot(lk[:, :bs], low)
            high, low = split(inner)
            out[r * bs : (r + 1) * bs, :] = dot(jnp.concatenate([high, low], axis=1), rcat[k]) + dot(high, rlow[k])
            t = jnp.where(r < held, tile[b], -1).astype(jnp.float32)
            meta = jnp.where(lane == r, jnp.where(row == 0, t, weight[k]), meta)
        out[CAP * bs :, :] = meta


def make_messages(steps, n_patch, me, dest, tile, expo, weight, blocks, left, right):
    bs = blocks.shape[1]
    shape = jax.ShapeDtypeStruct((CAP * bs + SUB, bs), jnp.float32)
    smem = pl.BlockSpec(memory_space=pltpu.SMEM)
    vmem = pl.BlockSpec(memory_space=pltpu.VMEM)
    n_k = left.shape[0]
    return pl.pallas_call(
        functools.partial(message_kernel, steps, n_patch),
        out_shape=[shape] * len(steps),
        in_specs=[smem] * 5 + [vmem] * 3,
        out_specs=[vmem] * len(steps),
        scratch_shapes=[
            pltpu.VMEM((n_k, bs, 2 * bs), jnp.bfloat16),
            pltpu.VMEM((n_k, 2 * bs, bs), jnp.bfloat16),
            pltpu.VMEM((n_k, bs, bs), jnp.bfloat16),
            pltpu.SMEM((n_patch * CAP,), jnp.int32),
            pltpu.SMEM((n_patch,), jnp.int32),
        ],
        cost_estimate=pl.CostEstimate(flops=len(steps) * CAP * 10 * bs**3, bytes_accessed=len(steps) * CAP * 8 * bs * bs, transcendentals=0),
        name="messages",
    )(me, dest, tile, expo, weight, blocks, left, right)


def meta_of(messages, bs):
    rows = jnp.concatenate([m[CAP * bs : CAP * bs + 2, :SUB] for m in messages], axis=0)
    rows = rows.reshape(len(messages), 2, SUB)
    return rows[:, 0, :CAP].reshape(-1).astype(jnp.int32), rows[:, 1, :CAP].reshape(-1)


def add_weights(tiles, weights, total, start):
    lane = lax.broadcasted_iota(jnp.int32, (SUB, LANES), 1)

    def one(s, acc):
        return acc + jnp.where(lane == tiles[s], weights[s], 0.0)

    return lax.fori_loop(0, total, one, start)


def sum_kernel(n, side, tiles, weights, *rest):
    messages, out = rest[:n], rest[n]
    bs = messages[0].shape[1]
    out[...] = jnp.zeros_like(out)
    out[side * bs :, :LANES] = add_weights(tiles, weights, n * CAP, jnp.zeros((SUB, LANES), jnp.float32))
    for m in range(n):
        for r in range(CAP):
            t = tiles[m * CAP + r]

            @pl.when(t >= 0)
            def _():
                rows = pl.ds(pl.multiple_of((t // side) * bs, bs), bs)
                cols = pl.ds(pl.multiple_of((t % side) * bs, bs), bs)
                out[rows, cols] += messages[m][r * bs : (r + 1) * bs, :]


def sum_messages(messages, side, bs):
    n = len(messages)
    tiles, weights = meta_of(messages, bs)
    smem = pl.BlockSpec(memory_space=pltpu.SMEM)
    vmem = pl.BlockSpec(memory_space=pltpu.VMEM)
    return pl.pallas_call(
        functools.partial(sum_kernel, n, side),
        out_shape=jax.ShapeDtypeStruct((side * bs + SUB, side * bs), jnp.float32),
        in_specs=[smem] * 2 + [vmem] * n,
        out_specs=vmem,
        cost_estimate=pl.CostEstimate(flops=n * CAP * bs * bs * 8, bytes_accessed=n * CAP * 4 * bs * bs, transcendentals=0),
        name="sums",
    )(tiles, weights, *messages)


def coadd_kernel(n, side, tiles, weights, mine, other, mine_w, other_w, *rest):
    messages = rest[:n]
    coadd, edge_rows, left, right, wsum = rest[n : n + 5]
    bs = messages[0].shape[1]
    i = pl.program_id(0)

    @pl.when(i == 0)
    def _():
        wsum[...] = 1.0 / (add_weights(tiles, weights, n * CAP, mine_w[:, :LANES] + other_w[:, :LANES]) + 1.0)

    coadd[...] = mine[...] + other[...]
    for m in range(n):
        for r in range(CAP):
            t = tiles[m * CAP + r]

            @pl.when((t >= 0) & (t // side == i))
            def _():
                cols = pl.ds(pl.multiple_of((t % side) * bs, bs), bs)
                coadd[:, cols] += messages[m][r * bs : (r + 1) * bs, :]

    lane = lax.broadcasted_iota(jnp.int32, (SUB, LANES), 1)
    inverse = wsum[...]
    for c in range(side):
        scale = jnp.sum(jnp.where(lane == i * side + c, inverse, 0.0), axis=1, keepdims=True)[:1]
        coadd[:, c * bs : (c + 1) * bs] = coadd[:, c * bs : (c + 1) * bs] * scale

    @pl.when(i == 0)
    def _():
        edge_rows[:SUB, :] = coadd[:SUB, :]

    @pl.when(i == side - 1)
    def _():
        edge_rows[SUB:, :] = coadd[bs - SUB :, :]

    left[...] = coadd[:, :bs].T[:SUB, :]
    right[...] = coadd[:, (side - 1) * bs :].T[bs - SUB :, :]


def finish_coadd(mine, other, messages, side, bs):
    n = len(messages)
    tiles, weights = meta_of(messages, bs)
    smem = pl.BlockSpec(memory_space=pltpu.SMEM)
    vmem = pl.BlockSpec(memory_space=pltpu.VMEM)
    width = side * bs
    band = pl.BlockSpec((bs, width), lambda i: (i, 0))
    tail = pl.BlockSpec((SUB, width), lambda i: (width // SUB, 0))
    strip = pl.BlockSpec((SUB, bs), lambda i: (0, i))
    out = jax.ShapeDtypeStruct
    return pl.pallas_call(
        functools.partial(coadd_kernel, n, side),
        grid=(side,),
        out_shape=[
            out((width, width), jnp.float32),
            out((2 * SUB, width), jnp.float32),
            out((SUB, width), jnp.float32),
            out((SUB, width), jnp.float32),
        ],
        in_specs=[smem] * 2 + [band, band, tail, tail] + [vmem] * n,
        out_specs=[band, pl.BlockSpec((2 * SUB, width), lambda i: (0, 0)), strip, strip],
        scratch_shapes=[pltpu.VMEM((SUB, LANES), jnp.float32)],
        cost_estimate=pl.CostEstimate(flops=width * width * 8, bytes_accessed=width * width * 12, transcendentals=0),
        name="coadd",
    )(tiles, weights, mine, other, mine, other, *messages)


def smooth_kernel(taps, above, below, west, east, before, band, after, out, west_cols, east_cols, padded):
    i = pl.program_id(0)
    n = pl.num_programs(0)
    bs, width = band.shape

    @pl.when(i == 0)
    def _():
        none = jnp.zeros((bs - SUB, bs), jnp.float32)
        for j in range(west.shape[1] // bs):
            at = slice(j * bs, (j + 1) * bs)
            west_cols[at, :] = jnp.concatenate([none, west[:, at]], axis=0).T
            east_cols[at, :] = jnp.concatenate([east[:, at], none], axis=0).T

    padded[:SUB, bs : bs + width] = jnp.where(i == 0, above[...], before[...])
    padded[SUB : SUB + bs, bs : bs + width] = band[...]
    padded[SUB + bs :, bs : bs + width] = jnp.where(i == n - 1, below[...], after[...])
    first = pl.multiple_of((i + 1) * bs - SUB, SUB)
    padded[:, :bs] = west_cols[pl.ds(first, bs + 2 * SUB), :]
    padded[:, bs + width :] = east_cols[pl.ds(first, bs + 2 * SUB), :]
    total = width + 2 * bs
    for r in range(0, bs, SUB):
        vertical = taps[HALO] * padded[r + SUB : r + 2 * SUB, :]
        for j in range(1, HALO + 1):
            vertical += taps[HALO + j] * (padded[r + SUB - j : r + 2 * SUB - j, :] + padded[r + SUB + j : r + 2 * SUB + j, :])
        result = taps[HALO] * vertical
        for j in range(1, HALO + 1):
            result += taps[HALO + j] * (pltpu.roll(vertical, j, 1) + pltpu.roll(vertical, total - j, 1))
        out[r : r + SUB, :] = result[:, bs : bs + width]


def smooth(coadd, taps, above, below, west, east, bs):
    width = coadd.shape[1]
    side = width // bs
    smem = pl.BlockSpec(memory_space=pltpu.SMEM)
    vmem = pl.BlockSpec(memory_space=pltpu.VMEM)
    per = bs // SUB
    band = pl.BlockSpec((bs, width), lambda i: (i, 0))
    return pl.pallas_call(
        smooth_kernel,
        grid=(side,),
        out_shape=jax.ShapeDtypeStruct((width, width), jnp.float32),
        in_specs=[smem, vmem, vmem, vmem, vmem]
        + [
            pl.BlockSpec((SUB, width), lambda i: (jnp.maximum(i * per - 1, 0), 0)),
            band,
            pl.BlockSpec((SUB, width), lambda i: (jnp.minimum((i + 1) * per, side * per - 1), 0)),
        ],
        out_specs=band,
        scratch_shapes=[
            pltpu.VMEM((width + 2 * bs, bs), jnp.float32),
            pltpu.VMEM((width + 2 * bs, bs), jnp.float32),
            pltpu.VMEM((bs + 2 * SUB, width + 2 * bs), jnp.float32),
        ],
        cost_estimate=pl.CostEstimate(flops=width * width * 36, bytes_accessed=width * width * 8, transcendentals=0),
        name="smooth",
    )(taps, above, below, west, east, coadd, coadd, coadd)


def flipped(value, axis, count, bit):
    return lax.ppermute(value, axis, [(i, i ^ bit) for i in range(count)])


def shifted(value, n_patch, rows, cols):
    pairs = []
    for source in range(n_patch):
        r, c = source // PCOLS + rows, source % PCOLS + cols
        if 0 <= r < n_patch // PCOLS and 0 <= c < PCOLS:
            pairs.append((source, r * PCOLS + c))
    return lax.ppermute(value, "patch", pairs) if pairs else jnp.zeros_like(value)


def body(n_exp, n_patch, pixels, exposure_of, destination, tile_slot, psf_left, psf_right, weights):
    blocks = pixels[0]
    bs = blocks.shape[1]
    side = PATCH_PIX // bs
    me = lax.axis_index("patch").astype(jnp.int32).reshape(1)
    scalars = (me, destination[0, :, 0], tile_slot[0], exposure_of[0], weights[0])
    make = lambda steps: make_messages(steps, n_patch, *scalars, blocks, psf_left[0], psf_right[0])
    half = n_patch // 2
    far = [*range(half + 1, n_patch), half]
    near = list(range(1, half))
    order = []
    for j in range(half):
        order += [far[j]] + near[2 * j : 2 * j + 2]
    order = [s for s in order if s < n_patch]
    sent = {}
    sent[order[0]] = make([order[0]])[0]
    others = [0, *order[1:]]
    for step, message in zip(others, make(others), strict=True):
        sent[step] = message
    got = {0: [sent[0]]}
    for step in order:
        got[step] = [flipped(sent[step], "patch", n_patch, step)]
    bit = n_exp // 2
    while bit > 1:
        for step in [0, *order]:
            got[step] = got[step] + [flipped(m, "exp", n_exp, bit) for m in got[step]]
        bit //= 2
    last = order[-1]
    early = [m for step in [0, *order[:-1]] for m in got[step]]
    mine = sum_messages(early, side, bs)
    other = flipped(mine, "exp", n_exp, 1)
    final = got[last] + [flipped(m, "exp", n_exp, 1) for m in got[last]]
    coadd, edge_rows, left, right = finish_coadd(mine, other, final, side, bs)
    above = shifted(edge_rows[SUB:], n_patch, 1, 0)
    below = shifted(edge_rows[:SUB], n_patch, -1, 0)
    west = jnp.concatenate(
        [shifted(right[:, -bs:], n_patch, 1, 1), shifted(right, n_patch, 0, 1), shifted(right[:, :bs], n_patch, -1, 1)],
        axis=1,
    )
    east = jnp.concatenate(
        [shifted(left[:, -bs:], n_patch, 1, -1), shifted(left, n_patch, 0, -1), shifted(left[:, :bs], n_patch, -1, -1)],
        axis=1,
    )
    detection = smooth(coadd, kernel_taps(), above, below, west, east, bs)
    return (coadd[None], detection[None])


def solution(mesh):
    return jax.shard_map(
        functools.partial(body, mesh.shape["exp"], mesh.shape["patch"]),
        mesh=mesh,
        in_specs=(
            P("exp", "patch", None, None),
            P("exp", "patch"),
            P("exp", "patch", None),
            P("exp", "patch"),
            P("exp", None, None, None),
            P("exp", None, None, None),
            P("exp", None),
        ),
        out_specs=(P("patch", None, None), P("patch", None, None)),
        check_vma=False,
    )
```

```python
import functools

import jax
import jax.numpy as jnp
import numpy as np
from jax import lax
from jax.experimental import pallas as pl
from jax.experimental.pallas import tpu as pltpu
from jax.sharding import PartitionSpec as P


PATCH_PIX = 1024
CAP = 6
HALO = 4
PCOLS = 4
SUB = 8
LANES = 128


def kernel_taps():
    taps = np.arange(-HALO, HALO + 1).astype(np.float32)
    values = np.exp(-taps * taps / np.float32(8.0))
    return [float(tap) for tap in values / np.sum(values)]


TAPS = kernel_taps()


def split(x):
    high = x.astype(jnp.bfloat16)
    return high, (x - high.astype(jnp.float32)).astype(jnp.bfloat16)


def dot(a, b):
    return jnp.dot(a, b, preferred_element_type=jnp.float32)


def message_kernel(steps, n_patch, *refs):
    given, refs = refs[:8], refs[8:]
    outs, refs = refs[: len(steps)], refs[len(steps) :]
    held, (lcat, rcat, rlow, slots, counts, sems) = refs[:8], refs[8:]
    copies = [pltpu.make_async_copy(a, b, sems.at[i]) for i, (a, b) in enumerate(zip(given, held, strict=True))]
    for copy in copies:
        copy.start()
    me, dest, tile, expo, weight, left, right, blocks = held
    count, bs = blocks.shape[0], blocks.shape[1]
    for q in range(n_patch):
        counts[q] = 0

    def place(b, carry):
        q = dest[b]
        r = counts[q]
        slots[q * CAP + r] = b
        counts[q] = r + 1
        return carry

    for copy in copies[:5]:
        copy.wait()
    lax.fori_loop(0, count, place, 0)
    for copy in copies[5:7]:
        copy.wait()
    for k in range(left.shape[0]):
        high, low = split(left[k] * weight[k])
        lcat[k, :, :bs] = high
        lcat[k, :, bs:] = low
        high, low = split(right[k].T)
        rcat[k, :bs, :] = high
        rcat[k, bs:, :] = high
        rlow[k] = low
    copies[7].wait()
    lane = lax.broadcasted_iota(jnp.int32, (SUB, LANES), 1)
    row = lax.broadcasted_iota(jnp.int32, (SUB, LANES), 0)
    for step, out in zip(steps, outs, strict=True):
        q = me[0] ^ step
        filled = counts[q]
        meta = jnp.where(row == CAP, -1.0, 0.0)
        for r in range(CAP):
            b = jnp.where(r < filled, slots[q * CAP + r], 0)
            k = expo[b]
            high, low = split(blocks[b])
            lk = lcat[k]
            inner = dot(lk, jnp.concatenate([high, high], axis=0)) + dot(lk[:, :bs], low)
            high, low = split(inner)
            out[r * bs : (r + 1) * bs, :] = dot(jnp.concatenate([high, low], axis=1), rcat[k]) + dot(high, rlow[k])
            t = jnp.where(r < filled, tile[b], -1)
            meta = jnp.where((row == r) & (lane == t), weight[k], meta)
            meta = jnp.where((row == CAP) & (lane == r), t.astype(jnp.float32), meta)
        out[CAP * bs :, :] = meta


def in_smem():
    return pl.BlockSpec(memory_space=pltpu.SMEM)


def in_vmem():
    return pl.BlockSpec(memory_space=pltpu.VMEM)


def params(mib):
    return pltpu.CompilerParams(vmem_limit_bytes=mib << 20)


def make_messages(steps, n_patch, me, dest, tile, expo, weight, left, right, blocks):
    bs = blocks.shape[1]
    shape = jax.ShapeDtypeStruct((CAP * bs + SUB, bs), jnp.float32)
    n_k = left.shape[0]
    given = (me, dest, tile, expo, weight, left, right, blocks)
    return pl.pallas_call(
        functools.partial(message_kernel, steps, n_patch),
        out_shape=[shape] * len(steps),
        in_specs=[pl.BlockSpec(memory_space=pltpu.HBM)] * len(given),
        out_specs=[in_vmem()] * len(steps),
        scratch_shapes=[
            *[pltpu.SMEM(a.shape, a.dtype) for a in given[:5]],
            *[pltpu.VMEM(a.shape, a.dtype) for a in given[5:]],
            pltpu.VMEM((n_k, bs, 2 * bs), jnp.bfloat16),
            pltpu.VMEM((n_k, 2 * bs, bs), jnp.bfloat16),
            pltpu.VMEM((n_k, bs, bs), jnp.bfloat16),
            pltpu.SMEM((n_patch * CAP,), jnp.int32),
            pltpu.SMEM((n_patch,), jnp.int32),
            pltpu.SemaphoreType.DMA((len(given),)),
        ],
        compiler_params=params(60),
        cost_estimate=pl.CostEstimate(flops=len(steps) * CAP * 10 * bs**3, bytes_accessed=len(steps) * CAP * 8 * bs * bs, transcendentals=0),
        name="messages",
    )(*given)


def add_messages(messages, side, out, tiles):
    bs = messages[0].shape[1]
    for m, message in enumerate(messages):
        for r in range(CAP):
            t = tiles[m, CAP, r].astype(jnp.int32)

            @pl.when(t >= 0)
            def _():
                rows = pl.ds(pl.multiple_of((t // side) * bs, bs), bs)
                cols = pl.ds(pl.multiple_of((t % side) * bs, bs), bs)
                out[rows, cols] += message[r * bs : (r + 1) * bs, :]


def fetch_tiles(messages, tiles, sems):
    bs = messages[0].shape[1]
    copies = [pltpu.make_async_copy(m.at[CAP * bs :, :], tiles.at[i], sems.at[i]) for i, m in enumerate(messages)]
    for copy in copies:
        copy.start()
    return copies


def tile_scratch(n):
    return [pltpu.SMEM((n, SUB, LANES), jnp.float32), pltpu.SemaphoreType.DMA((n,))]


def metas(messages):
    bs = messages[0].shape[1]
    total = messages[0][CAP * bs :, :]
    for m in messages[1:]:
        total += m[CAP * bs :, :]
    return total


def sum_kernel(n, side, *rest):
    messages, out, tiles, sems = rest[:n], *rest[n:]
    bs = messages[0].shape[1]
    copies = fetch_tiles(messages, tiles, sems)
    out[...] = jnp.zeros_like(out)
    out[side * bs :, :LANES] = metas(messages)
    for copy in copies:
        copy.wait()
    add_messages(messages, side, out, tiles)


def sum_messages(messages, side, bs):
    n = len(messages)
    return pl.pallas_call(
        functools.partial(sum_kernel, n, side),
        out_shape=jax.ShapeDtypeStruct((side * bs + SUB, side * bs), jnp.float32),
        in_specs=[in_vmem()] * n,
        out_specs=in_vmem(),
        scratch_shapes=tile_scratch(n),
        compiler_params=params(24),
        cost_estimate=pl.CostEstimate(flops=n * CAP * bs * bs * 8, bytes_accessed=n * CAP * 4 * bs * bs, transcendentals=0),
        name="sums",
    )(*messages)


def coadd_kernel(n, side, mine, other, *rest):
    messages = rest[:n]
    coadd, edge_rows, west, east, west_corners, east_corners, scale, tiles, sems = rest[n:]
    bs = messages[0].shape[1]
    width = side * bs
    copies = fetch_tiles(messages, tiles, sems)
    coadd[...] = mine[:width, :] + other[:width, :]
    total = metas(messages) + mine[width:, :LANES] + other[width:, :LANES]
    inverse = 1.0 / (jnp.sum(total[:CAP], axis=0, keepdims=True) + 1.0)
    scale[...] = jnp.broadcast_to(inverse, (LANES, LANES)).T
    for copy in copies:
        copy.wait()
    add_messages(messages, side, coadd, tiles)
    for t in range(side * side):
        at = (slice(t // side * bs, (t // side + 1) * bs), slice(t % side * bs, (t % side + 1) * bs))
        coadd[at] = coadd[at] * scale[t : t + 1, :]
    edge_rows[:SUB, :] = coadd[:SUB, :]
    edge_rows[SUB:, :] = coadd[width - SUB :, :]
    for i in range(side):
        at = slice(i * bs, (i + 1) * bs)
        west[:, at] = coadd[at, :bs].T[:SUB, :]
        east[:, at] = coadd[at, width - bs :].T[bs - SUB :, :]
    west_corners[:SUB, :] = west[:, :bs]
    west_corners[SUB:, :] = west[:, width - bs :]
    east_corners[:SUB, :] = east[:, :bs]
    east_corners[SUB:, :] = east[:, width - bs :]


def finish_coadd(mine, other, messages, side, bs):
    n = len(messages)
    width = side * bs
    shapes = [(width, width), (2 * SUB, width), (SUB, width), (SUB, width), (2 * SUB, bs), (2 * SUB, bs)]
    return pl.pallas_call(
        functools.partial(coadd_kernel, n, side),
        out_shape=[jax.ShapeDtypeStruct(shape, jnp.float32) for shape in shapes],
        in_specs=[in_vmem()] * (2 + n),
        out_specs=[in_vmem()] * len(shapes),
        scratch_shapes=[pltpu.VMEM((LANES, LANES), jnp.float32), *tile_scratch(n)],
        compiler_params=params(24),
        cost_estimate=pl.CostEstimate(flops=width * width * 8, bytes_accessed=width * width * 12, transcendentals=0),
        name="coadd",
    )(mine, other, *messages)


def smooth_kernel(rows, me, from_above, from_below, west, west_above, west_below, east, east_above, east_below, coadd, out, bands, west_cols, east_cols, vertical):
    i = pl.program_id(0)
    n = pl.num_programs(0)
    width = coadd.shape[1]
    bs = width // n
    total = width + 2 * bs
    row = me[0] // PCOLS
    has_above, has_below = row > 0, row < rows - 1

    @pl.when(i == 0)
    def _():
        none = jnp.zeros((bs - SUB, bs), jnp.float32)
        for j in range(total // bs):
            if j == 0:
                w, e = (jnp.where(has_above, ref[SUB:, :], 0.0) for ref in (west_above, east_above))
            elif j == total // bs - 1:
                w, e = (jnp.where(has_below, ref[:SUB, :], 0.0) for ref in (west_below, east_below))
            else:
                w, e = west[:, (j - 1) * bs : j * bs], east[:, (j - 1) * bs : j * bs]
            west_cols[j * bs : (j + 1) * bs, :] = jnp.concatenate([none, w], axis=0).T
            east_cols[j * bs : (j + 1) * bs, :] = jnp.concatenate([e, none], axis=0).T
        away = jnp.abs(lax.broadcasted_iota(jnp.int32, (bs, bs + 2 * SUB), 1) - lax.broadcasted_iota(jnp.int32, (bs, bs + 2 * SUB), 0) - SUB)
        g = jnp.zeros((bs, bs + 2 * SUB), jnp.float32)
        for j in range(HALO + 1):
            g = jnp.where(away == j, TAPS[HALO + j], g)
        bands[:bs, :], bands[bs:, :] = split(g)

    start = pl.multiple_of(i * bs, bs)
    before = pl.multiple_of(jnp.maximum(i * bs - SUB, 0), SUB)
    after = pl.multiple_of(jnp.minimum((i + 1) * bs, width - SUB), SUB)
    first = pl.multiple_of((i + 1) * bs - SUB, SUB)

    def filter_rows(at, columns):
        high, low = split(columns)
        both = dot(bands[...], high)
        vertical[:, at] = both[:bs] + both[bs:] + dot(bands[:bs, :], low)

    filter_rows(slice(0, bs), west_cols[pl.ds(first, bs + 2 * SUB), :])
    filter_rows(slice(total - bs, total), east_cols[pl.ds(first, bs + 2 * SUB), :])
    step = 2 * bs
    for c in range(0, width, step):
        at = slice(c, c + step)
        top = jnp.where(i == 0, jnp.where(has_above, from_above[SUB:, at], 0.0), coadd[pl.ds(before, SUB), at])
        bottom = jnp.where(i == n - 1, jnp.where(has_below, from_below[:SUB, at], 0.0), coadd[pl.ds(after, SUB), at])
        filter_rows(slice(bs + c, bs + c + step), jnp.concatenate([top, coadd[pl.ds(start, bs), at], bottom], axis=0))
    for r in range(0, bs, SUB):
        x = vertical[r : r + SUB, :]
        result = TAPS[HALO] * x
        for j in range(1, HALO + 1):
            result += TAPS[HALO + j] * (pltpu.roll(x, j, 1) + pltpu.roll(x, total - j, 1))
        out[r : r + SUB, :] = result[:, bs : bs + width]


def smooth(rows, me, halo, coadd, side):
    width = coadd.shape[1]
    bs = width // side
    return pl.pallas_call(
        functools.partial(smooth_kernel, rows),
        grid=(side,),
        out_shape=jax.ShapeDtypeStruct((width, width), jnp.float32),
        in_specs=[in_smem()] + [in_vmem()] * (len(halo) + 1),
        out_specs=pl.BlockSpec((bs, width), lambda i: (i, 0)),
        scratch_shapes=[
            pltpu.VMEM((2 * bs, bs + 2 * SUB), jnp.bfloat16),
            pltpu.VMEM((width + 2 * bs, bs), jnp.float32),
            pltpu.VMEM((width + 2 * bs, bs), jnp.float32),
            pltpu.VMEM((bs, width + 2 * bs), jnp.float32),
        ],
        compiler_params=params(24),
        cost_estimate=pl.CostEstimate(flops=width * width * 36, bytes_accessed=width * width * 8, transcendentals=0),
        name="smooth",
    )(me, *halo, coadd)


def flipped(value, axis, count, bit):
    return lax.ppermute(value, axis, [(i, i ^ bit) for i in range(count)])


def shifted(value, n_patch, rows, cols):
    pairs = []
    for source in range(n_patch):
        for step in rows:
            r, c = source // PCOLS + step, source % PCOLS + cols
            if 0 <= r < n_patch // PCOLS and 0 <= c < PCOLS:
                pairs.append((source, r * PCOLS + c))
    return lax.ppermute(value, "patch", pairs) if pairs else jnp.zeros_like(value)


def both_ways(value, n_patch, cols):
    if n_patch == 2 * PCOLS:
        one = shifted(value, n_patch, (1, -1), cols)
        return one, one
    return shifted(value, n_patch, (1,), cols), shifted(value, n_patch, (-1,), cols)


def step_order(n_patch):
    half = n_patch // 2
    far, near = [*range(half + 1, n_patch), half], list(range(1, half))
    order = []
    for j in range(half):
        order += [far[j], *near[2 * j : 2 * j + 2]]
    return order


LATE = 2


def body(n_exp, n_patch, pixels, exposure_of, destination, tile_slot, psf_left, psf_right, weights):
    blocks = pixels[0]
    bs = blocks.shape[1]
    side = PATCH_PIX // bs
    me = lax.axis_index("patch").astype(jnp.int32).reshape(1)
    order = step_order(n_patch)
    steps = [0, *order]
    made = make_messages(steps, n_patch, me, destination[0, :, 0], tile_slot[0], exposure_of[0], weights[0], psf_left[0], psf_right[0], blocks)
    sent = dict(zip(steps, made, strict=True))
    got = {0: [sent[0]]}
    for step in order:
        got[step] = [flipped(sent[step], "patch", n_patch, step)]
    bit = n_exp // 2
    while bit > 1:
        for step in steps:
            got[step] = got[step] + [flipped(m, "exp", n_exp, bit) for m in got[step]]
        bit //= 2
    early = [m for step in steps[:-LATE] for m in got[step]]
    mine = sum_messages(early, side, bs)
    other = flipped(mine, "exp", n_exp, 1)
    late = [m for step in steps[-LATE:] for m in got[step]]
    final = late + [flipped(m, "exp", n_exp, 1) for m in late]
    coadd, edge_rows, west, east, west_corners, east_corners = finish_coadd(mine, other, final, side, bs)
    from_above, from_below = both_ways(edge_rows, n_patch, 0)
    west_above, west_below = both_ways(east_corners, n_patch, 1)
    east_above, east_below = both_ways(west_corners, n_patch, -1)
    from_west = shifted(east, n_patch, (0,), 1)
    from_east = shifted(west, n_patch, (0,), -1)
    halo = (from_above, from_below, from_west, west_above, west_below, from_east, east_above, east_below)
    detection = smooth(n_patch // PCOLS, me, halo, coadd, side)
    return (coadd[None], detection[None])


def solution(mesh):
    n_exp, n_patch = mesh.shape["exp"], mesh.shape["patch"]
    return jax.shard_map(
        functools.partial(body, n_exp, n_patch),
        mesh=mesh,
        in_specs=(
            P("exp", "patch", None, None),
            P("exp", "patch"),
            P("exp", "patch", None),
            P("exp", "patch"),
            P("exp", None, None, None),
            P("exp", None, None, None),
            P("exp", None),
        ),
        out_specs=(P("patch", None, None), P("patch", None, None)),
        check_vma=False,
    )
```
